32 devices in a mesh: layer: 4 (over y, x), row: 2 (over core), col: 4 (over z).
Axes of the slice: x: 2, y: 2, z: 4, core: 2. Of those that a mesh axis runs over, the one named last changes fastest.
Arguments:
- block_values: bfloat16 [4, 2, 4, 32, 256, 256], P('layer', 'row', 'col'), may hold values from 0 to 3
- block_rows: int32 [4, 2, 4, 32], P('layer', 'row', 'col'), may hold values from 0 to 255
- block_cols: int32 [4, 2, 4, 32], P('layer', 'row', 'col'), may hold values from 0 to 127
- block_count: int32 [4, 2, 4], P('layer', 'row', 'col'), may hold values from 1 to 32, as said below
- dangling: int32 [4, 2, 4, 16384], P('layer', 'row', 'col'), may hold values 0 or 1
- start_ranks: float32 [4, 2, 4, 16384], P('layer', 'row', 'col'), may hold values from 0.2 to 5
Outputs:
- ranks: float32 [4, 2, 4, 16384], P('layer', 'row', 'col')
- residuals: float32 [3, 4], P(None, 'layer')
The draws below stay inside these ranges and needn't reach their ends.
Inputs may be any that keep to these rules, and one draw needn't show every extreme that they name: `block_count`: live slots of a tile; in every layer some tile has all 32 slots live. `block_rows`: slots at or past a tile's count carry no edges; coordinates may repeat within a tile, and repeated blocks add.
All inputs are finite; a program needn't handle non-finite values. No bound on the sum of `dangling` on one device may be relied on, other than what follows from the above.
Results may differ from the reference program's by a relative error of at most 0.0012.
Values may be sent and summed in bfloat16 or wider, within the bound.
A program may use at most 64 MiB of HBM per device.

```python
import math
import jax
import jax.numpy as jnp
from jax import lax

BLOCK = 256
MAXB = 32
ITERS = 3
ROW_BLK = 256
LAYERS = 4
NODES = 131072
SPAN = 16384
COL_BLK = 128
N_ROW = 2
N_COL = 4


def draw_block_values(key, part):
    shape = (LAYERS, N_ROW, N_COL, MAXB, BLOCK, BLOCK)
    first_key = jax.random.fold_in(jax.random.fold_in(key, 11), 0)
    values = jnp.exp(jax.random.uniform(first_key, shape, jnp.float32, math.log(0.05), 0.0))
    return values.astype(jnp.bfloat16)


def draw_block_count(key, part):
    first_key, second_key = jax.random.split(jax.random.fold_in(key, 23))
    tiles = N_ROW * N_COL
    counts = jax.random.randint(first_key, (LAYERS, tiles), max(1, MAXB // 4), MAXB + 1, jnp.int32)
    fullest = jax.random.randint(second_key, (LAYERS, 1), 0, tiles, jnp.int32)
    counts = jnp.where(jnp.arange(tiles, dtype=jnp.int32)[None, :] == fullest, MAXB, counts)
    return counts.reshape(LAYERS, N_ROW, N_COL).astype(jnp.int32)


def touch_ends(values, rng, low, largest):
    dims = values.shape
    index_at = [jax.random.randint(jax.random.fold_in(rng, axis), (), 0, dims[axis]) for axis in range(len(dims))]
    values = values.at[tuple(index_at)].set(low)
    longest = dims.index(max(dims))
    index_at[longest] = (index_at[longest] + 1) % dims[longest]
    return values.at[tuple(index_at)].set(largest)


def steps_of(rng, dims, cuts, smallest, largest):
    level, own = 1.0, jax.random.fold_in(rng, 6)
    for axis_at, parts in cuts:
        draws = jnp.exp(jax.random.uniform(jax.random.fold_in(own, axis_at), (parts,), jnp.float32, smallest / len(cuts), largest / len(cuts)))
        level = level * jnp.repeat(draws, dims[axis_at] // parts).reshape([-1 if axis == axis_at else 1 for axis in range(len(dims))])
    return level


def setup_inputs(seed: int = 0) -> dict:
    arg_keys = jax.random.split(jax.random.key(seed), 7)
    return {
        "block_values": draw_block_values(jax.random.fold_in(arg_keys[6], 71), 0),
        "block_rows": touch_ends(jax.random.randint(arg_keys[1], (LAYERS, N_ROW, N_COL, MAXB), 0, ROW_BLK), jax.random.fold_in(arg_keys[1], 1), 0, ROW_BLK - 1).astype(jnp.int32),
        "block_cols": touch_ends(jax.random.randint(arg_keys[2], (LAYERS, N_ROW, N_COL, MAXB), 0, COL_BLK), jax.random.fold_in(arg_keys[2], 1), 0, COL_BLK - 1).astype(jnp.int32),
        "block_count": draw_block_count(jax.random.fold_in(arg_keys[6], 71), 0),
        "dangling": touch_ends((jax.random.randint(arg_keys[4], (LAYERS, N_ROW, N_COL, SPAN), 0, 8) < 1).astype(jnp.int32), jax.random.fold_in(arg_keys[4], 1), 0, 1),
        "start_ranks": jnp.clip(jnp.exp(math.log(5.0) - 3.218876 * jax.random.uniform(arg_keys[5], (LAYERS, N_ROW, N_COL, SPAN), jnp.float32) ** steps_of(arg_keys[5], (LAYERS, N_ROW, N_COL, SPAN), ((0, 4), (1, 2), (2, 4)), -0.2, 0.2)), 0.2, 5.0),
    }


damping = 0.85
coupling = 0.3


def reference(block_values, block_rows, block_cols, block_count, dangling, start_ranks):
    live_slot = (jnp.arange(MAXB)[None, None, None, :] < block_count[..., None]).astype(jnp.float32)

    def degree_layer(packed):
        values, cols_here, live_here = packed
        colsum = jnp.einsum('rcsij->rcsj', values.astype(jnp.float32))
        onehot = (cols_here[..., None] == jnp.arange(COL_BLK)[None, None, None, :]).astype(jnp.float32) * live_here[..., None]
        deg_group = jnp.einsum('rcsb,rcsj->cbj', onehot, colsum, precision=lax.Precision.HIGHEST)
        return jnp.transpose(deg_group.reshape(N_COL, N_ROW, SPAN), (1, 0, 2))

    degree = lax.map(degree_layer, (block_values, block_cols, live_slot))
    keep_mask = 1.0 - dangling.astype(jnp.float32)
    denominator = keep_mask * degree + 1.0
    layer_ids = jnp.arange(LAYERS)
    spread = jnp.where((layer_ids == 0) | (layer_ids == LAYERS - 1), 1.0, 0.5).astype(jnp.float32) * coupling
    spread = spread.reshape(LAYERS, 1, 1, 1)

    def walk_layer(packed):
        values, rows_here, cols_here, live_here, scaled_here = packed
        column_bf = jnp.transpose(scaled_here, (1, 0, 2)).reshape(N_COL, COL_BLK, BLOCK)
        picked = column_bf[jnp.arange(N_COL)[None, :, None], cols_here]
        products = jnp.einsum('rcsij,rcsj->rcsi', values.astype(jnp.float32), picked.astype(jnp.float32))
        onehot = (rows_here[..., None] == jnp.arange(ROW_BLK)[None, None, None, :]).astype(jnp.float32) * live_here[..., None]
        walk_sum = jnp.einsum('rcsb,rcsi->rbi', onehot, products, precision=lax.Precision.HIGHEST)
        return walk_sum.reshape(N_ROW, N_COL, SPAN)

    ranks_now = start_ranks
    residual_list = []
    for iteration in range(ITERS):
        scaled = (ranks_now * keep_mask / denominator).astype(jnp.bfloat16)
        walk_sum = lax.map(walk_layer, (block_values, block_rows, block_cols, live_slot, scaled))
        dangle_mass = jnp.sum(ranks_now / denominator, axis=(1, 2, 3), keepdims=True)
        spill = ranks_now * spread
        padded = jnp.pad(spill, ((1, 1), (0, 0), (0, 0), (0, 0)))
        arrive = padded[:-2] + padded[2:]
        updated = damping * ((1.0 - coupling) * (walk_sum + dangle_mass / NODES) + arrive) + (1.0 - damping)
        residual_list.append(jnp.sum(jnp.abs(updated - ranks_now), axis=(1, 2, 3)))
        ranks_now = updated
    return ranks_now, jnp.stack(residual_list)
```

```python
import functools

import jax
import jax.numpy as jnp
from jax import lax
from jax.experimental import pallas as pl
from jax.experimental.pallas import tpu as pltpu
from jax.sharding import PartitionSpec as P

ITERS = 3
CHUNK = 16

damping = 0.85
coupling = 0.3


def fold(v):
    rows, lanes = v.shape
    acc = v[:, 0:128]
    for h in range(1, lanes // 128):
        acc = acc + v[:, h * 128 : (h + 1) * 128]
    return jnp.sum(acc.reshape(rows // 8, 8, 128), axis=0)


def split(v):
    hi = v.astype(jnp.bfloat16)
    lo = (v - hi.astype(jnp.float32)).astype(jnp.bfloat16)
    return hi, lo


def dot(a, b):
    return jnp.dot(a, b, preferred_element_type=jnp.float32)


def kernel(
    nl, nr, nc, nodes,
    values_hbm, rows_ref, cols_ref, count_ref, dang_hbm, start_hbm,
    ranks_hbm, resid_ref,
    values, dang_in, start_in, out_buf, x_ref, inv_ref, kinv_ref, keep_ref,
    colsum, ohrow, ohcol, own_prod, chg,
    deg_send, deg_recv, row_send, row_recv,
    sc_send, sc_recv, ma_send, ma_recv, mb_send, mb_recv,
    pr_send, pr_recv, sp_send, sp_recv, rs_send, rs_recv,
    sem_in, sem_v,
    deg_ss, deg_rs, row_ss, row_rs, sc_ss, sc_rs, ma_ss, ma_rs, mb_ss, mb_rs,
    pr_ss, pr_rs, sp_ss, sp_rs, rs_ss, rs_rs,
):
    l, r, c = (lax.axis_index(a) for a in ("layer", "row", "col"))
    slots, edge, _ = values.shape
    blocks = x_ref.shape[0]
    halves = edge // 128
    nchunk = slots // CHUNK
    f32, bf16 = jnp.float32, jnp.bfloat16

    def remote(src, dst, ss, rs, ll, rr, cc):
        return pltpu.make_async_remote_copy(
            src_ref=src, dst_ref=dst, send_sem=ss, recv_sem=rs,
            device_id=(ll, rr, cc), device_id_type=pl.DeviceIdType.MESH,
        )

    in_d = pltpu.make_async_copy(dang_hbm, dang_in, sem_in.at[0])
    in_x = pltpu.make_async_copy(start_hbm, start_in, sem_in.at[1])
    vcopies = [
        pltpu.make_async_copy(
            values_hbm.at[pl.ds(k * CHUNK, CHUNK)], values.at[pl.ds(k * CHUNK, CHUNK)], sem_v.at[k]
        )
        for k in range(nchunk)
    ]
    for cp in vcopies:
        cp.start()
    in_x.start()
    in_d.start()

    peers = [(dr, dc) for dr in range(nr) for dc in range(nc) if (dr, dc) != (0, 0)]
    barrier = pltpu.get_barrier_semaphore()
    for dr, dc in peers:
        pl.semaphore_signal(
            barrier, inc=1,
            device_id=(l, lax.rem(r + dr, nr), lax.rem(c + dc, nc)),
            device_id_type=pl.DeviceIdType.MESH,
        )

    @pl.when(l > 0)
    def _():
        pl.semaphore_signal(
            barrier, inc=1, device_id=(l - 1, r, c), device_id_type=pl.DeviceIdType.MESH)

    @pl.when(l < nl - 1)
    def _():
        pl.semaphore_signal(
            barrier, inc=1, device_id=(l + 1, r, c), device_id_type=pl.DeviceIdType.MESH)

    live = lax.broadcasted_iota(jnp.int32, (1, slots), 1) < count_ref[0]
    rows = jnp.where(live, rows_ref[...], -1)
    cols = jnp.where(live, cols_ref[...], -1)
    row_send[...] = jnp.broadcast_to(
        jnp.concatenate([rows, jnp.full((1, 128 - slots), -1, jnp.int32)], axis=1), (8, 128)
    ).astype(f32)

    eye = lax.broadcasted_iota(jnp.int32, (slots, slots), 0) == lax.broadcasted_iota(
        jnp.int32, (slots, slots), 1)
    colv = jnp.sum(
        jnp.where(eye, jnp.broadcast_to(cols_ref[...], (slots, slots)).astype(f32), 0.0),
        axis=1, keepdims=True,
    )
    for d in range(nr):
        base = lax.rem(r - d + nr, nr) * blocks
        at = (lax.broadcasted_iota(jnp.int32, (slots, blocks), 1) + base).astype(f32)
        ohcol[d] = jnp.where(colv == at, 1.0, 0.0).astype(bf16)

    ones = jnp.ones((CHUNK, edge), bf16)
    rid = lax.broadcasted_iota(jnp.int32, (CHUNK, edge), 0)
    for k in range(nchunk):
        vcopies[k].wait()
        acc = jnp.zeros((CHUNK, edge), f32)
        for s in range(CHUNK):
            acc = jnp.where(rid == s, dot(ones, values[k * CHUNK + s]), acc)
        colsum[k * CHUNK : (k + 1) * CHUNK] = acc

    in_x.wait()
    in_d.wait()
    for h in range(halves):
        x_ref[:, h * 128 : (h + 1) * 128] = start_in[pl.ds(h, blocks, stride=halves), :]
        keep_ref[:, h * 128 : (h + 1) * 128] = 1.0 - dang_in[
            pl.ds(h, blocks, stride=halves), :].astype(f32)

    hi, lo = split(colsum[...])

    def deg_of(rr):
        base = rr * blocks
        at = lax.broadcasted_iota(jnp.int32, (blocks, slots), 0) + base
        oh = jnp.where(jnp.broadcast_to(cols, (blocks, slots)) == at, 1.0, 0.0).astype(bf16)
        return dot(oh, hi) + dot(oh, lo)

    for d in range(1, nr):
        deg_send[d] = deg_of(lax.rem(r + d, nr))

    pl.semaphore_wait(
        barrier, len(peers) + (l > 0).astype(jnp.int32) + (l < nl - 1).astype(jnp.int32))

    pre = []
    for d in range(1, nr):
        pre.append(remote(deg_send.at[d], deg_recv.at[d], deg_ss.at[d], deg_rs.at[d],
                          l, lax.rem(r + d, nr), c))
    for d in range(1, nc):
        pre.append(remote(row_send, row_recv.at[d], row_ss.at[d], row_rs.at[d],
                          l, r, lax.rem(c + d, nc)))
    for cp in pre:
        cp.start()

    def spill_copies(t):
        return (
            remote(sp_send.at[t], sp_recv.at[t, 0], sp_ss.at[t, 0], sp_rs.at[t, 0], l + 1, r, c),
            remote(sp_send.at[t], sp_recv.at[t, 1], sp_ss.at[t, 1], sp_rs.at[t, 1], l - 1, r, c),
        )

    spread = jnp.where((l == 0) | (l == nl - 1), 1.0, 0.5).astype(f32) * coupling

    def send_spill(t, x):
        sp_send[t] = (x * spread).astype(sp_send.dtype)
        up, down = spill_copies(t)

        @pl.when(l < nl - 1)
        def _():
            up.start()

        @pl.when(l > 0)
        def _():
            down.start()

    @pl.when(l == 0)
    def _():
        for t in range(ITERS):
            sp_recv[t, 0] = jnp.zeros((blocks, edge), sp_recv.dtype)

    @pl.when(l == nl - 1)
    def _():
        for t in range(ITERS):
            sp_recv[t, 1] = jnp.zeros((blocks, edge), sp_recv.dtype)

    send_spill(0, x_ref[...])

    deg = deg_of(r)
    for d in range(1, nr):
        pre[d - 1].wait_recv()
        deg = deg + deg_recv[d]
    keep = keep_ref[...]
    inv = 1.0 / (keep * deg + 1.0)
    inv_ref[...] = inv
    kinv_ref[...] = keep * inv

    def row_onehot(tab):
        at = (lax.broadcasted_iota(jnp.int32, (blocks, slots), 0) + c * blocks).astype(f32)
        return jnp.where(jnp.broadcast_to(tab[0:1, 0:slots], (blocks, slots)) == at,
                         1.0, 0.0).astype(bf16)

    chg[...] = jnp.zeros((8, 128), f32)

    def step(t, _):
        x = x_ref[...]
        scaled = (x * kinv_ref[...]).astype(bf16)
        sc_send[t] = scaled
        sc = [
            remote(sc_send.at[t], sc_recv.at[t, d], sc_ss.at[t, d], sc_rs.at[t, d],
                   l, lax.rem(r + d, nr), c)
            for d in range(1, nr)
        ]
        for cp in sc:
            cp.start()
        mass_own = fold(x * inv_ref[...])
        ma_send[t] = mass_own
        ma = [
            remote(ma_send.at[t], ma_recv.at[t, d], ma_ss.at[t, d], ma_rs.at[t, d],
                   l, lax.rem(r + d, nr), c)
            for d in range(1, nr)
        ]
        for cp in ma:
            cp.start()

        @pl.when(t > 0)
        def _():
            send_spill(t, x_ref[...])

        picked = dot(ohcol[0], scaled)
        for d in range(1, nr):
            sc[d - 1].wait_recv()
            picked = picked + dot(ohcol[d], sc_recv[t, d])
        picked = picked.astype(bf16)

        pr = []
        for k in range(nchunk):
            lhs = picked[k * CHUNK : (k + 1) * CHUNK]
            acc = jnp.zeros((CHUNK, edge), f32)
            for s in range(CHUNK):
                res = lax.dot_general(
                    lhs, values[k * CHUNK + s], (((1,), (1,)), ((), ())),
                    preferred_element_type=f32)
                acc = jnp.where(rid == s, res, acc)
            own_prod[k * CHUNK : (k + 1) * CHUNK] = acc
            pr_send[t, k] = acc.astype(pr_send.dtype)
            for d in range(1, nc):
                cp = remote(pr_send.at[t, k], pr_recv.at[t, d, k], pr_ss.at[t, d, k],
                            pr_rs.at[t, d, k], l, r, lax.rem(c + d, nc))
                cp.start()
                pr.append((d, k, cp))

        mass_row = mass_own
        for d in range(1, nr):
            ma[d - 1].wait_recv()
            mass_row = mass_row + ma_recv[t, d]
        mb_send[t] = mass_row
        mb = [
            remote(mb_send.at[t], mb_recv.at[t, d], mb_ss.at[t, d], mb_rs.at[t, d],
                   l, r, lax.rem(c + d, nc))
            for d in range(1, nc)
        ]
        for cp in mb:
            cp.start()

        @pl.when(t == 0)
        def _():
            ohrow[0] = row_onehot(row_send)
            for d in range(1, nc):
                pre[nr - 1 + d - 1].wait_recv()
                ohrow[d] = row_onehot(row_recv[d])

        phi, plo = split(own_prod[...])
        walk = dot(ohrow[0], phi) + dot(ohrow[0], plo)

        up, down = spill_copies(t)

        @pl.when(l > 0)
        def _():
            up.wait_recv()

        @pl.when(l < nl - 1)
        def _():
            down.wait_recv()

        arrive = sp_recv[t, 0].astype(f32) + sp_recv[t, 1].astype(f32)
        mass = mass_row
        for d in range(1, nc):
            mb[d - 1].wait_recv()
            mass = mass + mb_recv[t, d]
        rest = damping * ((1.0 - coupling) * (jnp.sum(mass) / nodes) + arrive) + (1.0 - damping)

        for d, k, cp in pr:
            cp.wait_recv()
        for d in range(1, nc):
            got = pr_recv[t, d].reshape(slots, edge)
            if got.dtype == bf16:
                walk = walk + dot(ohrow[d], got)
            else:
                ghi, glo = split(got)
                walk = walk + dot(ohrow[d], ghi) + dot(ohrow[d], glo)
        updated = damping * (1.0 - coupling) * walk + rest
        x_ref[...] = updated
        change = jnp.sum(fold(jnp.abs(updated - x)))
        lane = lax.broadcasted_iota(jnp.int32, (8, 128), 1)
        chg[...] = jnp.where(lane == t, change, chg[...])

        for cp in sc + ma + mb + [p[2] for p in pr]:
            cp.wait_send()

        @pl.when(l < nl - 1)
        def _():
            up.wait_send()

        @pl.when(l > 0)
        def _():
            down.wait_send()

        return 0

    lax.fori_loop(0, ITERS, step, 0)

    rs_send[...] = chg[0:1]
    rs = []
    for i, (dr, dc) in enumerate(peers):
        cp = remote(rs_send, rs_recv.at[i], rs_ss.at[i], rs_rs.at[i],
                    l, lax.rem(r + dr, nr), lax.rem(c + dc, nc))
        cp.start()
        rs.append(cp)
    for h in range(halves):
        out_buf[pl.ds(h, blocks, stride=halves), :] = x_ref[:, h * 128 : (h + 1) * 128]
    out = pltpu.make_async_copy(out_buf, ranks_hbm, sem_in.at[0])
    out.start()
    for cp in pre:
        cp.wait_send()
    total = rs_send[...]
    for i, cp in enumerate(rs):
        cp.wait_recv()
        total = total + rs_recv[i]
    pick = lax.broadcasted_iota(jnp.int32, (ITERS, 128), 0) == lax.broadcasted_iota(
        jnp.int32, (ITERS, 128), 1)
    resid_ref[...] = jnp.sum(
        jnp.where(pick, jnp.broadcast_to(total, (ITERS, 128)), 0.0), axis=1, keepdims=True)
    for cp in rs:
        cp.wait_send()
    out.wait()


def local(block_values, block_rows, block_cols, block_count, dangling, start_ranks):
    span = start_ranks.shape[-1]
    nl, nr, nc = (lax.axis_size(a) for a in ("layer", "row", "col"))
    slots, edge = block_values.shape[3], block_values.shape[-1]
    blocks = span // edge
    nchunk = slots // CHUNK
    nodes = nr * nc * span
    npeer = nr * nc - 1
    f32, bf16 = jnp.float32, jnp.bfloat16
    vm, dma = pltpu.VMEM, pltpu.SemaphoreType.DMA
    big = (blocks, edge)
    PT, ST = bf16, f32
    scratch = [
        vm((slots, edge, edge), bf16), vm((span // 128, 128), jnp.int32), vm((span // 128, 128), f32),
        vm((span // 128, 128), f32), vm(big, f32), vm(big, f32), vm(big, f32), vm(big, f32),
        vm((slots, edge), f32), vm((nc, blocks, slots), bf16), vm((nr, slots, blocks), bf16),
        vm((slots, edge), f32), vm((8, 128), f32),
        vm((nr,) + big, f32), vm((nr,) + big, f32), vm((8, 128), f32), vm((nc, 8, 128), f32),
        vm((ITERS,) + big, bf16), vm((ITERS, nr) + big, bf16),
        vm((ITERS, 8, 128), f32), vm((ITERS, nr, 8, 128), f32),
        vm((ITERS, 8, 128), f32), vm((ITERS, nc, 8, 128), f32),
        vm((ITERS, nchunk, CHUNK, edge), PT), vm((ITERS, nc, nchunk, CHUNK, edge), PT),
        vm((ITERS,) + big, ST), vm((ITERS, 2) + big, ST),
        vm((1, 128), f32), vm((npeer, 1, 128), f32),
        dma((2,)), dma((nchunk,)),
        dma((nr,)), dma((nr,)), dma((nc,)), dma((nc,)),
        dma((ITERS, nr)), dma((ITERS, nr)), dma((ITERS, nr)), dma((ITERS, nr)),
        dma((ITERS, nc)), dma((ITERS, nc)),
        dma((ITERS, nc, nchunk)), dma((ITERS, nc, nchunk)),
        dma((ITERS, 2)), dma((ITERS, 2)), dma((npeer,)), dma((npeer,)),
    ]
    hbm = pl.BlockSpec(memory_space=pl.ANY)
    vmem = pl.BlockSpec(memory_space=pltpu.VMEM)
    smem = pl.BlockSpec(memory_space=pltpu.SMEM)
    ranks, resid = pl.pallas_call(
        functools.partial(kernel, nl, nr, nc, nodes),
        out_shape=(
            jax.ShapeDtypeStruct((span // 128, 128), f32),
            jax.ShapeDtypeStruct((ITERS, 1), f32),
        ),
        in_specs=[hbm, vmem, vmem, smem, hbm, hbm],
        out_specs=(hbm, vmem),
        scratch_shapes=scratch,
        compiler_params=pltpu.CompilerParams(collective_id=0, has_side_effects=True),
    )(
        block_values.reshape(slots, edge, edge),
        block_rows.reshape(1, slots),
        block_cols.reshape(1, slots),
        block_count.reshape(1),
        dangling.reshape(span // 128, 128),
        start_ranks.reshape(span // 128, 128),
    )
    return ranks.reshape(1, 1, 1, span), resid


def solution(mesh):
    placed = (
        P("layer", "row", "col", None, None, None),
        P("layer", "row", "col", None),
        P("layer", "row", "col", None),
        P("layer", "row", "col"),
        P("layer", "row", "col", None),
        P("layer", "row", "col", None),
    )
    return jax.shard_map(
        local,
        mesh=mesh,
        in_specs=placed,
        out_specs=(P("layer", "row", "col", None), P(None, "layer")),
        check_vma=False,
    )
```

```python
import functools

import jax
import jax.numpy as jnp
from jax import lax
from jax.experimental import pallas as pl
from jax.experimental.pallas import tpu as pltpu
from jax.sharding import PartitionSpec as P

ITERS = 3
CHUNK = 16

damping = 0.85
coupling = 0.3


def fold(v):
    rows, lanes = v.shape
    acc = v[:, 0:128]
    for h in range(1, lanes // 128):
        acc = acc + v[:, h * 128 : (h + 1) * 128]
    return jnp.sum(acc.reshape(rows // 8, 8, 128), axis=0)


def split(v):
    hi = v.astype(jnp.bfloat16)
    lo = (v - hi.astype(jnp.float32)).astype(jnp.bfloat16)
    return hi, lo


def dot(a, b):
    return jnp.dot(a, b, preferred_element_type=jnp.float32)


def kernel(
    nl, nr, nc, nodes,
    values_hbm, rows_ref, cols_ref, count_ref, dang_hbm, start_hbm,
    ranks_hbm, resid_ref,
    values, dang_in, start_in, out_buf, x_ref, inv_ref, kinv_ref,
    colsum, ohrow, ohcol, own_prod, chg,
    px_recv, pd_recv, col_send, col_recv, cs_recv, row_send, row_recv,
    sc_send, sc_recv, ma_send, ma_recv, mb_send, mb_recv,
    pr_send, pr_recv, sp_send, sp_recv, rs_send, rs_recv,
    sem_in, sem_v,
    px_ss, px_rs, pd_ss, pd_rs, col_ss, col_rs, cs_ss, cs_rs, row_ss, row_rs, sc_ss, sc_rs, ma_ss, ma_rs, mb_ss, mb_rs,
    pr_ss, pr_rs, sp_ss, sp_rs, rs_ss, rs_rs,
):
    l, r, c = (lax.axis_index(a) for a in ("layer", "row", "col"))
    slots, edge, _ = values.shape
    blocks = x_ref.shape[0]
    halves = edge // 128
    nchunk = slots // CHUNK
    f32, bf16 = jnp.float32, jnp.bfloat16

    def remote(src, dst, ss, rs, ll, rr, cc):
        return pltpu.make_async_remote_copy(
            src_ref=src, dst_ref=dst, send_sem=ss, recv_sem=rs,
            device_id=(ll, rr, cc), device_id_type=pl.DeviceIdType.MESH,
        )

    in_d = pltpu.make_async_copy(dang_hbm, dang_in, sem_in.at[0])
    in_x = pltpu.make_async_copy(start_hbm, start_in, sem_in.at[1])
    vcopies = [
        pltpu.make_async_copy(
            values_hbm.at[pl.ds(k * CHUNK, CHUNK)], values.at[pl.ds(k * CHUNK, CHUNK)], sem_v.at[k]
        )
        for k in range(nchunk)
    ]
    in_x.start()
    in_d.start()
    for cp in vcopies:
        cp.start()

    peers = [(dr, dc) for dr in range(nr) for dc in range(nc) if (dr, dc) != (0, 0)]
    barrier = pltpu.get_barrier_semaphore()
    for dr, dc in peers:
        pl.semaphore_signal(
            barrier, inc=1,
            device_id=(l, lax.rem(r + dr, nr), lax.rem(c + dc, nc)),
            device_id_type=pl.DeviceIdType.MESH,
        )

    @pl.when(l > 0)
    def _():
        pl.semaphore_signal(
            barrier, inc=1, device_id=(l - 1, r, c), device_id_type=pl.DeviceIdType.MESH)

    @pl.when(l < nl - 1)
    def _():
        pl.semaphore_signal(
            barrier, inc=1, device_id=(l + 1, r, c), device_id_type=pl.DeviceIdType.MESH)

    live = lax.broadcasted_iota(jnp.int32, (1, slots), 1) < count_ref[0]
    rows = jnp.where(live, rows_ref[...], -1)
    cols = jnp.where(live, cols_ref[...], -1)
    row_send[...] = jnp.broadcast_to(
        jnp.concatenate([rows, jnp.full((1, 128 - slots), -1, jnp.int32)], axis=1), (8, 128)
    ).astype(f32)
    col_send[...] = jnp.broadcast_to(
        jnp.concatenate([cols, jnp.full((1, 128 - slots), -1, jnp.int32)], axis=1), (8, 128)
    ).astype(f32)

    eye = lax.broadcasted_iota(jnp.int32, (slots, slots), 0) == lax.broadcasted_iota(
        jnp.int32, (slots, slots), 1)
    colv = jnp.sum(
        jnp.where(eye, jnp.broadcast_to(cols_ref[...], (slots, slots)).astype(f32), 0.0),
        axis=1, keepdims=True,
    )
    for d in range(nr):
        base = lax.rem(r - d + nr, nr) * blocks
        at = (lax.broadcasted_iota(jnp.int32, (slots, blocks), 1) + base).astype(f32)
        ohcol[d] = jnp.where(colv == at, 1.0, 0.0).astype(bf16)

    ones = jnp.ones((CHUNK, edge), bf16)
    rid = lax.broadcasted_iota(jnp.int32, (CHUNK, edge), 0)

    def column_sum(k):
        vcopies[k].wait()
        acc = jnp.zeros((CHUNK, edge), f32)
        for s in range(CHUNK):
            acc = jnp.where(rid == s, dot(ones, values[k * CHUNK + s]), acc)
        colsum[k] = acc

    in_x.wait()
    in_d.wait()
    for h in range(halves):
        x_ref[:, h * 128 : (h + 1) * 128] = start_in[pl.ds(h, blocks, stride=halves), :]
    column_sum(0)

    order = []
    first, last = jnp.int32(0), jnp.int32(nc - 1)
    for _ in range(nc - 1):
        left = (c - first >= last - c).astype(jnp.int32)
        order.append(left * first + (1 - left) * last)
        first, last = first + left, last - (1 - left)
    far = [(cc, lax.rem(cc - c + nc, nc)) for cc in order]

    pl.semaphore_wait(
        barrier, len(peers) + (l > 0).astype(jnp.int32) + (l < nl - 1).astype(jnp.int32))

    px, pd, pc, pcs, prow = [], [], [], [], []
    for d in range(1, nr):
        rr = lax.rem(r + d, nr)
        px.append(remote(start_in, px_recv.at[d], px_ss.at[d], px_rs.at[d], l, rr, c))
        pd.append(remote(dang_in, pd_recv.at[d], pd_ss.at[d], pd_rs.at[d], l, rr, c))
        pc.append(remote(col_send, col_recv.at[d], col_ss.at[d], col_rs.at[d], l, rr, c))
        pcs.append([
            remote(colsum.at[k], cs_recv.at[d, k], cs_ss.at[d, k], cs_rs.at[d, k], l, rr, c)
            for k in range(nchunk)
        ])
    for cc, d in far:
        prow.append(remote(row_send, row_recv.at[d], row_ss.at[d], row_rs.at[d], l, r, cc))
    for cp in px + pd + pc + prow + [q[0] for q in pcs]:
        cp.start()

    def spill_copies(t):
        return (
            remote(sp_send.at[t], sp_recv.at[t, 0], sp_ss.at[t, 0], sp_rs.at[t, 0], l + 1, r, c),
            remote(sp_send.at[t], sp_recv.at[t, 1], sp_ss.at[t, 1], sp_rs.at[t, 1], l - 1, r, c),
        )

    spread = jnp.where((l == 0) | (l == nl - 1), 1.0, 0.5).astype(f32) * coupling

    def send_spill(t, x):
        sp_send[t] = (x * spread).astype(sp_send.dtype)
        up, down = spill_copies(t)

        @pl.when(l < nl - 1)
        def _():
            up.start()

        @pl.when(l > 0)
        def _():
            down.start()

    @pl.when(l == 0)
    def _():
        for t in range(ITERS):
            sp_recv[t, 0] = jnp.zeros((blocks, edge), sp_recv.dtype)

    @pl.when(l == nl - 1)
    def _():
        for t in range(ITERS):
            sp_recv[t, 1] = jnp.zeros((blocks, edge), sp_recv.dtype)

    send_spill(0, x_ref[...])

    for k in range(1, nchunk):
        column_sum(k)
        for q in pcs:
            q[k].start()

    def spread_sums(tab, sums, rr):
        at = (lax.broadcasted_iota(jnp.int32, (blocks, slots), 0) + rr * blocks).astype(f32)
        oh = jnp.where(
            jnp.broadcast_to(tab[0:1, 0:slots], (blocks, slots)) == at, 1.0, 0.0).astype(bf16)
        hi, lo = split(sums.reshape(slots, edge))
        return dot(oh, hi) + dot(oh, lo)

    def piece(buf, h):
        return buf[pl.ds(h, blocks, stride=halves), :]

    near = [spread_sums(col_send, colsum[...], lax.rem(r - d + nr, nr)) for d in range(nr)]
    for cp in px + pd + pc:
        cp.wait_recv()
    peer_x = {d: jnp.concatenate([piece(px_recv.at[d], h) for h in range(halves)], axis=1)
              for d in range(1, nr)}
    keeps = {d: 1.0 - jnp.concatenate(
        [piece(pd_recv.at[d] if d else dang_in, h) for h in range(halves)], axis=1).astype(f32)
        for d in range(nr)}
    for q in pcs:
        for cp in q:
            cp.wait_recv()
    for d in range(nr):
        deg = near[d]
        for e in range(1, nr):
            deg = deg + spread_sums(col_recv[e], cs_recv[e], lax.rem(r - d + nr, nr))
        inv = 1.0 / (keeps[d] * deg + 1.0)
        kinv = keeps[d] * inv
        if d == 0:
            inv_ref[...] = inv
            kinv_ref[...] = kinv
        else:
            sc_recv[0, d] = (peer_x[d] * kinv).astype(bf16)

    def row_onehot(tab):
        at = (lax.broadcasted_iota(jnp.int32, (blocks, slots), 0) + c * blocks).astype(f32)
        return jnp.where(jnp.broadcast_to(tab[0:1, 0:slots], (blocks, slots)) == at,
                         1.0, 0.0).astype(bf16)

    def step(t):
        x = x_ref[...]
        scaled = (x * kinv_ref[...]).astype(bf16)
        if t > 0:
            sc_send[t] = scaled
        sc = [
            remote(sc_send.at[t], sc_recv.at[t, d], sc_ss.at[t, d], sc_rs.at[t, d],
                   l, lax.rem(r + d, nr), c)
            for d in range(1, nr)
            if t > 0
        ]
        for cp in sc:
            cp.start()
        mass_own = fold(x * inv_ref[...])
        ma_send[t] = mass_own
        ma = [
            remote(ma_send.at[t], ma_recv.at[t, d], ma_ss.at[t, d], ma_rs.at[t, d],
                   l, lax.rem(r + d, nr), c)
            for d in range(1, nr)
        ]
        for cp in ma:
            cp.start()

        if t > 0:
            send_spill(t, x)

        picked = dot(ohcol[0], scaled)
        for d in range(1, nr):
            if t > 0:
                sc[d - 1].wait_recv()
            picked = picked + dot(ohcol[d], sc_recv[t, d])
        picked = picked.astype(bf16)

        pr = []
        for k in range(nchunk):
            lhs = picked[k * CHUNK : (k + 1) * CHUNK]
            acc = jnp.zeros((CHUNK, edge), f32)
            for s in range(CHUNK):
                res = lax.dot_general(
                    lhs, values[k * CHUNK + s], (((1,), (1,)), ((), ())),
                    preferred_element_type=f32)
                acc = jnp.where(rid == s, res, acc)
            own_prod[k * CHUNK : (k + 1) * CHUNK] = acc
            pr_send[t, k] = acc.astype(pr_send.dtype)
            for cc, d in far:
                cp = remote(pr_send.at[t, k], pr_recv.at[t, d, k], pr_ss.at[t, d, k],
                            pr_rs.at[t, d, k], l, r, cc)
                cp.start()
                pr.append(cp)

        mass_row = mass_own
        for d in range(1, nr):
            ma[d - 1].wait_recv()
            mass_row = mass_row + ma_recv[t, d]
        mb_send[t] = mass_row
        mb = [
            remote(mb_send.at[t], mb_recv.at[t, d], mb_ss.at[t, d], mb_rs.at[t, d],
                   l, r, cc)
            for cc, d in far
        ]
        for cp in mb:
            cp.start()

        if t == 0:
            ohrow[0] = row_onehot(row_send)
            for cp in prow:
                cp.wait_recv()
            for d in range(1, nc):
                ohrow[d] = row_onehot(row_recv[d])

        phi, plo = split(own_prod[...])
        walk = dot(ohrow[0], phi) + dot(ohrow[0], plo)

        up, down = spill_copies(t)

        @pl.when(l > 0)
        def _():
            up.wait_recv()

        @pl.when(l < nl - 1)
        def _():
            down.wait_recv()

        arrive = sp_recv[t, 0].astype(f32) + sp_recv[t, 1].astype(f32)
        mass = mass_row
        for cp in mb:
            cp.wait_recv()
        for d in range(1, nc):
            mass = mass + mb_recv[t, d]
        rest = damping * ((1.0 - coupling) * (jnp.sum(mass) / nodes) + arrive) + (1.0 - damping)

        for cp in pr:
            cp.wait_recv()
        for d in range(1, nc):
            got = pr_recv[t, d].reshape(slots, edge)
            if got.dtype == bf16:
                walk = walk + dot(ohrow[d], got)
            else:
                ghi, glo = split(got)
                walk = walk + dot(ohrow[d], ghi) + dot(ohrow[d], glo)
        updated = damping * (1.0 - coupling) * walk + rest
        x_ref[...] = updated
        chg[t] = fold(jnp.abs(updated - x))

        for cp in sc + ma + mb + pr:
            cp.wait_send()

        @pl.when(l < nl - 1)
        def _():
            up.wait_send()

        @pl.when(l > 0)
        def _():
            down.wait_send()

    for t in range(ITERS):
        step(t)

    lane = lax.broadcasted_iota(jnp.int32, (1, 128), 1)
    changes = jnp.zeros((1, 128), f32)
    for t in range(ITERS):
        changes = jnp.where(lane == t, jnp.sum(chg[t]), changes)
    rs_send[...] = changes
    rs = []
    for i, (dr, dc) in enumerate(peers):
        cp = remote(rs_send, rs_recv.at[i], rs_ss.at[i], rs_rs.at[i],
                    l, lax.rem(r + dr, nr), lax.rem(c + dc, nc))
        cp.start()
        rs.append(cp)
    for h in range(halves):
        out_buf[pl.ds(h, blocks, stride=halves), :] = x_ref[:, h * 128 : (h + 1) * 128]
    out = pltpu.make_async_copy(out_buf, ranks_hbm, sem_in.at[0])
    out.start()
    for cp in px + pd + pc + prow + [e for q in pcs for e in q]:
        cp.wait_send()
    total = rs_send[...]
    for i, cp in enumerate(rs):
        cp.wait_recv()
        total = total + rs_recv[i]
    resid_ref[...] = total
    for cp in rs:
        cp.wait_send()
    out.wait()


def finish(ranks_in, resid_in, ranks_ref, resid_ref):
    ranks_ref[...] = ranks_in[...]
    resid_ref[...] = resid_in[:, 0:ITERS]


def local(block_values, block_rows, block_cols, block_count, dangling, start_ranks):
    span = start_ranks.shape[-1]
    nl, nr, nc = (lax.axis_size(a) for a in ("layer", "row", "col"))
    slots, edge = block_values.shape[3], block_values.shape[-1]
    blocks = span // edge
    nchunk = slots // CHUNK
    nodes = nr * nc * span
    npeer = nr * nc - 1
    f32, bf16 = jnp.float32, jnp.bfloat16
    vm, dma = pltpu.VMEM, pltpu.SemaphoreType.DMA
    big = (blocks, edge)
    PT, ST = bf16, f32
    scratch = [
        vm((slots, edge, edge), bf16), vm((span // 128, 128), jnp.int32), vm((span // 128, 128), f32),
        vm((span // 128, 128), f32), vm(big, f32), vm(big, f32), vm(big, f32),
        vm((nchunk, CHUNK, edge), f32), vm((nc, blocks, slots), bf16), vm((nr, slots, blocks), bf16),
        vm((slots, edge), f32), vm((ITERS, 8, 128), f32),
        vm((nr, span // 128, 128), f32), vm((nr, span // 128, 128), jnp.int32),
        vm((8, 128), f32), vm((nr, 8, 128), f32), vm((nr, nchunk, CHUNK, edge), f32),
        vm((8, 128), f32), vm((nc, 8, 128), f32),
        vm((ITERS,) + big, bf16), vm((ITERS, nr) + big, bf16),
        vm((ITERS, 8, 128), f32), vm((ITERS, nr, 8, 128), f32),
        vm((ITERS, 8, 128), f32), vm((ITERS, nc, 8, 128), f32),
        vm((ITERS, nchunk, CHUNK, edge), PT), vm((ITERS, nc, nchunk, CHUNK, edge), PT),
        vm((ITERS,) + big, ST), vm((ITERS, 2) + big, ST),
        vm((1, 128), f32), vm((npeer, 1, 128), f32),
        dma((2,)), dma((nchunk,)),
        dma((nr,)), dma((nr,)), dma((nr,)), dma((nr,)), dma((nr,)), dma((nr,)),
        dma((nr, nchunk)), dma((nr, nchunk)), dma((nc,)), dma((nc,)),
        dma((ITERS, nr)), dma((ITERS, nr)), dma((ITERS, nr)), dma((ITERS, nr)),
        dma((ITERS, nc)), dma((ITERS, nc)),
        dma((ITERS, nc, nchunk)), dma((ITERS, nc, nchunk)),
        dma((ITERS, 2)), dma((ITERS, 2)), dma((npeer,)), dma((npeer,)),
    ]
    hbm = pl.BlockSpec(memory_space=pl.ANY)
    vmem = pl.BlockSpec(memory_space=pltpu.VMEM)
    smem = pl.BlockSpec(memory_space=pltpu.SMEM)
    ranks, resid = pl.pallas_call(
        functools.partial(kernel, nl, nr, nc, nodes),
        out_shape=(
            jax.ShapeDtypeStruct((span // 128, 128), f32),
            jax.ShapeDtypeStruct((1, 128), f32),
        ),
        in_specs=[hbm, vmem, vmem, smem, hbm, hbm],
        out_specs=(hbm, vmem),
        scratch_shapes=scratch,
        compiler_params=pltpu.CompilerParams(collective_id=0, has_side_effects=True),
    )(
        block_values.reshape(slots, edge, edge),
        block_rows.reshape(1, slots),
        block_cols.reshape(1, slots),
        block_count.reshape(1),
        dangling.reshape(span // 128, 128),
        start_ranks.reshape(span // 128, 128),
    )
    ranks, resid = pl.pallas_call(
        finish,
        out_shape=(
            jax.ShapeDtypeStruct((span // 128, 128), f32),
            jax.ShapeDtypeStruct((1, ITERS), f32),
        ),
        in_specs=[vmem, vmem],
        out_specs=(vmem, vmem),
    )(ranks, resid)
    return ranks.reshape(1, 1, 1, span), resid.T


def solution(mesh):
    placed = (
        P("layer", "row", "col", None, None, None),
        P("layer", "row", "col", None),
        P("layer", "row", "col", None),
        P("layer", "row", "col"),
        P("layer", "row", "col", None),
        P("layer", "row", "col", None),
    )
    return jax.shard_map(
        local,
        mesh=mesh,
        in_specs=placed,
        out_specs=(P("layer", "row", "col", None), P(None, "layer")),
        check_vma=False,
    )
```

```python
import functools

import jax
import jax.numpy as jnp
from jax import lax
from jax.experimental import pallas as pl
from jax.experimental.pallas import tpu as pltpu
from jax.sharding import PartitionSpec as P

ITERS = 3
CHUNK = 16

damping = 0.85
coupling = 0.3


def fold(v):
    rows, lanes = v.shape
    acc = v[:, 0:128]
    for h in range(1, lanes // 128):
        acc = acc + v[:, h * 128 : (h + 1) * 128]
    return jnp.sum(acc.reshape(rows // 8, 8, 128), axis=0)


def split(v):
    hi = v.astype(jnp.bfloat16)
    lo = (v - hi.astype(jnp.float32)).astype(jnp.bfloat16)
    return hi, lo


def dot(a, b):
    return jnp.dot(a, b, preferred_element_type=jnp.float32)


def kernel(
    nl, nr, nc, nodes,
    values_hbm, rows_ref, cols_ref, count_ref, dang_hbm, start_hbm,
    ranks_ref, resid_ref,
    values, dang_in, start_in, x_ref, inv_ref, kinv_ref,
    colsum, ohrow, ohcol, own_prod, chg,
    px_recv, pd_recv, col_send, col_recv, cs_recv, row_send, row_recv,
    sc_send, sc_recv, ma_send, ma_recv,
    pr_send, pr_recv, sp_send, sp_recv, rs_send, rs_recv,
    sem_in, sem_v,
    px_ss, px_rs, pd_ss, pd_rs, col_ss, col_rs, cs_ss, cs_rs, row_ss, row_rs, sc_ss, sc_rs, ma_ss, ma_rs,
    pr_ss, pr_rs, sp_ss, sp_rs, rs_ss, rs_rs,
):
    l, r, c = (lax.axis_index(a) for a in ("layer", "row", "col"))
    slots, edge, _ = values.shape
    blocks = x_ref.shape[0]
    halves = edge // 128
    nchunk = slots // CHUNK
    f32, bf16 = jnp.float32, jnp.bfloat16

    def remote(src, dst, ss, rs, ll, rr, cc):
        return pltpu.make_async_remote_copy(
            src_ref=src, dst_ref=dst, send_sem=ss, recv_sem=rs,
            device_id=(ll, rr, cc), device_id_type=pl.DeviceIdType.MESH,
        )

    in_d = pltpu.make_async_copy(dang_hbm, dang_in, sem_in.at[0])
    in_x = pltpu.make_async_copy(start_hbm, start_in, sem_in.at[1])
    vcopies = [
        pltpu.make_async_copy(
            values_hbm.at[pl.ds(k * CHUNK, CHUNK)], values.at[pl.ds(k * CHUNK, CHUNK)], sem_v.at[k]
        )
        for k in range(nchunk)
    ]
    in_x.start()
    in_d.start()
    for cp in vcopies:
        cp.start()

    peers = [(dr, dc) for dr in range(nr) for dc in range(nc) if (dr, dc) != (0, 0)]
    barrier = pltpu.get_barrier_semaphore()
    for dr, dc in peers:
        pl.semaphore_signal(
            barrier, inc=1,
            device_id=(l, lax.rem(r + dr, nr), lax.rem(c + dc, nc)),
            device_id_type=pl.DeviceIdType.MESH,
        )

    @pl.when(l > 0)
    def _():
        pl.semaphore_signal(
            barrier, inc=1, device_id=(l - 1, r, c), device_id_type=pl.DeviceIdType.MESH)

    @pl.when(l < nl - 1)
    def _():
        pl.semaphore_signal(
            barrier, inc=1, device_id=(l + 1, r, c), device_id_type=pl.DeviceIdType.MESH)

    live = lax.broadcasted_iota(jnp.int32, (1, slots), 1) < count_ref[0]
    rows = jnp.where(live, rows_ref[...], -1)
    cols = jnp.where(live, cols_ref[...], -1)
    row_send[...] = jnp.broadcast_to(
        jnp.concatenate([rows, jnp.full((1, 128 - slots), -1, jnp.int32)], axis=1), (8, 128)
    ).astype(f32)
    col_send[...] = jnp.broadcast_to(
        jnp.concatenate([cols, jnp.full((1, 128 - slots), -1, jnp.int32)], axis=1), (8, 128)
    ).astype(f32)

    eye = lax.broadcasted_iota(jnp.int32, (slots, slots), 0) == lax.broadcasted_iota(
        jnp.int32, (slots, slots), 1)
    colv = jnp.sum(
        jnp.where(eye, jnp.broadcast_to(cols_ref[...], (slots, slots)).astype(f32), 0.0),
        axis=1, keepdims=True,
    )
    for d in range(nr):
        base = lax.rem(r - d + nr, nr) * blocks
        at = (lax.broadcasted_iota(jnp.int32, (slots, blocks), 1) + base).astype(f32)
        ohcol[d] = jnp.where(colv == at, 1.0, 0.0).astype(bf16)

    ones = jnp.ones((CHUNK, edge), bf16)
    rid = lax.broadcasted_iota(jnp.int32, (CHUNK, edge), 0)

    def column_sum(k):
        vcopies[k].wait()
        acc = jnp.zeros((CHUNK, edge), f32)
        for s in range(CHUNK):
            acc = jnp.where(rid == s, dot(ones, values[k * CHUNK + s]), acc)
        colsum[k] = acc

    in_x.wait()
    in_d.wait()
    for h in range(halves):
        x_ref[:, h * 128 : (h + 1) * 128] = start_in[pl.ds(h, blocks, stride=halves), :]
    column_sum(0)

    order = []
    first, last = jnp.int32(0), jnp.int32(nc - 1)
    for _ in range(nc - 1):
        left = (c - first >= last - c).astype(jnp.int32)
        order.append(left * first + (1 - left) * last)
        first, last = first + left, last - (1 - left)
    far = [(cc, lax.rem(cc - c + nc, nc)) for cc in order]
    far_peers = [(dr, cc, d) for cc, d in far for dr in range(nr)]
    far_peers += [(dr, c, 0) for dr in range(1, nr)]
    sent = []

    pl.semaphore_wait(
        barrier, len(peers) + (l > 0).astype(jnp.int32) + (l < nl - 1).astype(jnp.int32))

    px, pd, pc, pcs, prow = [], [], [], [], []
    for d in range(1, nr):
        rr = lax.rem(r + d, nr)
        px.append(remote(start_in, px_recv.at[d], px_ss.at[d], px_rs.at[d], l, rr, c))
        pd.append(remote(dang_in, pd_recv.at[d], pd_ss.at[d], pd_rs.at[d], l, rr, c))
        pc.append(remote(col_send, col_recv.at[d], col_ss.at[d], col_rs.at[d], l, rr, c))
        pcs.append([
            remote(colsum.at[k], cs_recv.at[d, k], cs_ss.at[d, k], cs_rs.at[d, k], l, rr, c)
            for k in range(nchunk)
        ])
    for cc, d in far:
        prow.append(remote(row_send, row_recv.at[d], row_ss.at[d], row_rs.at[d], l, r, cc))
    for cp in px + pd + pc + prow + [q[0] for q in pcs]:
        cp.start()

    def spill_copies(t):
        return (
            remote(sp_send.at[t], sp_recv.at[t, 0], sp_ss.at[t, 0], sp_rs.at[t, 0], l + 1, r, c),
            remote(sp_send.at[t], sp_recv.at[t, 1], sp_ss.at[t, 1], sp_rs.at[t, 1], l - 1, r, c),
        )

    spread = jnp.where((l == 0) | (l == nl - 1), 1.0, 0.5).astype(f32) * coupling

    def send_spill(t, x):
        sp_send[t] = (x * spread).astype(sp_send.dtype)
        up, down = spill_copies(t)

        @pl.when(l < nl - 1)
        def _():
            up.start()

        @pl.when(l > 0)
        def _():
            down.start()

    @pl.when(l == 0)
    def _():
        for t in range(ITERS):
            sp_recv[t, 0] = jnp.zeros((blocks, edge), sp_recv.dtype)

    @pl.when(l == nl - 1)
    def _():
        for t in range(ITERS):
            sp_recv[t, 1] = jnp.zeros((blocks, edge), sp_recv.dtype)

    send_spill(0, x_ref[...])

    for k in range(1, nchunk):
        column_sum(k)
        for q in pcs:
            q[k].start()

    def spread_sums(tab, sums, rr):
        at = (lax.broadcasted_iota(jnp.int32, (blocks, slots), 0) + rr * blocks).astype(f32)
        oh = jnp.where(
            jnp.broadcast_to(tab[0:1, 0:slots], (blocks, slots)) == at, 1.0, 0.0).astype(bf16)
        hi, lo = split(sums.reshape(slots, edge))
        return dot(oh, hi) + dot(oh, lo)

    def piece(buf, h):
        return buf[pl.ds(h, blocks, stride=halves), :]

    near = [spread_sums(col_send, colsum[...], lax.rem(r - d + nr, nr)) for d in range(nr)]
    for cp in px + pd + pc:
        cp.wait_recv()
    peer_x = {d: jnp.concatenate([piece(px_recv.at[d], h) for h in range(halves)], axis=1)
              for d in range(1, nr)}
    keeps = {d: 1.0 - jnp.concatenate(
        [piece(pd_recv.at[d] if d else dang_in, h) for h in range(halves)], axis=1).astype(f32)
        for d in range(nr)}
    for q in pcs:
        for cp in q:
            cp.wait_recv()
    for d in range(nr):
        deg = near[d]
        for e in range(1, nr):
            deg = deg + spread_sums(col_recv[e], cs_recv[e], lax.rem(r - d + nr, nr))
        inv = 1.0 / (keeps[d] * deg + 1.0)
        kinv = keeps[d] * inv
        if d == 0:
            inv_ref[...] = inv
            kinv_ref[...] = kinv
        else:
            sc_recv[0, d] = (peer_x[d] * kinv).astype(bf16)

    def row_onehot(tab):
        at = (lax.broadcasted_iota(jnp.int32, (blocks, slots), 0) + c * blocks).astype(f32)
        return jnp.where(jnp.broadcast_to(tab[0:1, 0:slots], (blocks, slots)) == at,
                         1.0, 0.0).astype(bf16)

    def step(t):
        x = x_ref[...]
        scaled = (x * kinv_ref[...]).astype(bf16)
        if t > 0:
            sc_send[t] = scaled
        sc = [
            remote(sc_send.at[t], sc_recv.at[t, d], sc_ss.at[t, d], sc_rs.at[t, d],
                   l, lax.rem(r + d, nr), c)
            for d in range(1, nr)
            if t > 0
        ]
        for cp in sc:
            cp.start()
        mass_own = jnp.sum(fold(x * inv_ref[...]), axis=0, keepdims=True)
        ma_send[t] = mass_own
        ma = []
        for i, (dr, cc, dc) in enumerate(far_peers):
            slot = dr * nc + dc - 1
            ma.append(remote(ma_send.at[t], ma_recv.at[t, slot], ma_ss.at[t, slot],
                             ma_rs.at[t, slot], l, lax.rem(r + dr, nr), cc))
        for cp in ma:
            cp.start()

        if t > 0:
            send_spill(t, x)

        picked = dot(ohcol[0], scaled)
        for d in range(1, nr):
            if t > 0:
                sc[d - 1].wait_recv()
            picked = picked + dot(ohcol[d], sc_recv[t, d])
        picked = picked.astype(bf16)

        pr = []
        for k in range(nchunk):
            lhs = picked[k * CHUNK : (k + 1) * CHUNK]
            acc = jnp.zeros((CHUNK, edge), f32)
            for s in range(CHUNK):
                res = lax.dot_general(
                    lhs, values[k * CHUNK + s], (((1,), (1,)), ((), ())),
                    preferred_element_type=f32)
                acc = jnp.where(rid == s, res, acc)
            own_prod[k * CHUNK : (k + 1) * CHUNK] = acc
            pr_send[t, k] = acc.astype(pr_send.dtype)
            for cc, d in far:
                cp = remote(pr_send.at[t, k], pr_recv.at[t, d, k], pr_ss.at[t, d, k],
                            pr_rs.at[t, d, k], l, r, cc)
                cp.start()
                pr.append(cp)

        if t == 0:
            ohrow[0] = row_onehot(row_send)
            for cp in prow:
                cp.wait_recv()
            for d in range(1, nc):
                ohrow[d] = row_onehot(row_recv[d])

        phi, plo = split(own_prod[...])
        walk = dot(ohrow[0], phi) + dot(ohrow[0], plo)

        up, down = spill_copies(t)

        @pl.when(l > 0)
        def _():
            up.wait_recv()

        @pl.when(l < nl - 1)
        def _():
            down.wait_recv()

        arrive = sp_recv[t, 0].astype(f32) + sp_recv[t, 1].astype(f32)
        mass = mass_own
        for cp in ma:
            cp.wait_recv()
        for i in range(len(peers)):
            mass = mass + ma_recv[t, i]
        rest = damping * ((1.0 - coupling) * (jnp.sum(mass) / nodes) + arrive) + (1.0 - damping)

        for cp in pr:
            cp.wait_recv()
        for d in range(1, nc):
            got = pr_recv[t, d].reshape(slots, edge)
            if got.dtype == bf16:
                walk = walk + dot(ohrow[d], got)
            else:
                ghi, glo = split(got)
                walk = walk + dot(ohrow[d], ghi) + dot(ohrow[d], glo)
        updated = damping * (1.0 - coupling) * walk + rest
        x_ref[...] = updated
        chg[t] = fold(jnp.abs(updated - x))

        sent.extend(sc + ma + pr)

    for t in range(ITERS):
        step(t)

    lane = lax.broadcasted_iota(jnp.int32, (1, 128), 1)
    changes = jnp.zeros((1, 128), f32)
    for t in range(ITERS):
        changes = jnp.where(lane == t, jnp.sum(chg[t]), changes)
    rs_send[...] = changes
    rs = []
    for i, (dr, dc) in enumerate(peers):
        cp = remote(rs_send, rs_recv.at[i], rs_ss.at[i], rs_rs.at[i],
                    l, lax.rem(r + dr, nr), lax.rem(c + dc, nc))
        cp.start()
        rs.append(cp)
    for h in range(halves):
        ranks_ref[pl.ds(h, blocks, stride=halves), :] = x_ref[:, h * 128 : (h + 1) * 128]
    for cp in px + pd + pc + prow + [e for q in pcs for e in q] + sent:
        cp.wait_send()
    ups = [spill_copies(t) for t in range(ITERS)]

    @pl.when(l < nl - 1)
    def _():
        for up, _ in ups:
            up.wait_send()

    @pl.when(l > 0)
    def _():
        for _, down in ups:
            down.wait_send()

    total = rs_send[...]
    for i, cp in enumerate(rs):
        cp.wait_recv()
        total = total + rs_recv[i]
    resid_ref[...] = total
    for cp in rs:
        cp.wait_send()


def finish(ranks_in, resid_in, ranks_ref, resid_ref):
    ranks_ref[...] = ranks_in[...]
    resid_ref[...] = resid_in[:, 0:ITERS]


def local(block_values, block_rows, block_cols, block_count, dangling, start_ranks):
    span = start_ranks.shape[-1]
    nl, nr, nc = (lax.axis_size(a) for a in ("layer", "row", "col"))
    slots, edge = block_values.shape[3], block_values.shape[-1]
    blocks = span // edge
    nchunk = slots // CHUNK
    nodes = nr * nc * span
    npeer = nr * nc - 1
    f32, bf16 = jnp.float32, jnp.bfloat16
    vm, dma = pltpu.VMEM, pltpu.SemaphoreType.DMA
    big = (blocks, edge)
    PT, ST = bf16, f32
    scratch = [
        vm((slots, edge, edge), bf16), vm((span // 128, 128), jnp.int32), vm((span // 128, 128), f32),
        vm(big, f32), vm(big, f32), vm(big, f32),
        vm((nchunk, CHUNK, edge), f32), vm((nc, blocks, slots), bf16), vm((nr, slots, blocks), bf16),
        vm((slots, edge), f32), vm((ITERS, 8, 128), f32),
        vm((nr, span // 128, 128), f32), vm((nr, span // 128, 128), jnp.int32),
        vm((8, 128), f32), vm((nr, 8, 128), f32), vm((nr, nchunk, CHUNK, edge), f32),
        vm((8, 128), f32), vm((nc, 8, 128), f32),
        vm((ITERS,) + big, bf16), vm((ITERS, nr) + big, bf16),
        vm((ITERS, 1, 128), f32), vm((ITERS, npeer, 1, 128), f32),
        vm((ITERS, nchunk, CHUNK, edge), PT), vm((ITERS, nc, nchunk, CHUNK, edge), PT),
        vm((ITERS,) + big, ST), vm((ITERS, 2) + big, ST),
        vm((1, 128), f32), vm((npeer, 1, 128), f32),
        dma((2,)), dma((nchunk,)),
        dma((nr,)), dma((nr,)), dma((nr,)), dma((nr,)), dma((nr,)), dma((nr,)),
        dma((nr, nchunk)), dma((nr, nchunk)), dma((nc,)), dma((nc,)),
        dma((ITERS, nr)), dma((ITERS, nr)), dma((ITERS, npeer)), dma((ITERS, npeer)),
        dma((ITERS, nc, nchunk)), dma((ITERS, nc, nchunk)),
        dma((ITERS, 2)), dma((ITERS, 2)), dma((npeer,)), dma((npeer,)),
    ]
    hbm = pl.BlockSpec(memory_space=pltpu.HBM)
    vmem = pl.BlockSpec(memory_space=pltpu.VMEM)
    smem = pl.BlockSpec(memory_space=pltpu.SMEM)
    ranks, resid = pl.pallas_call(
        functools.partial(kernel, nl, nr, nc, nodes),
        out_shape=(
            pltpu.VMEM((span // 128, 128), f32),
            pltpu.VMEM((1, 128), f32),
        ),
        in_specs=[hbm, vmem, vmem, smem, hbm, hbm],
        out_specs=(vmem, vmem),
        scratch_shapes=scratch,
        compiler_params=pltpu.CompilerParams(collective_id=0, has_side_effects=True),
    )(
        block_values.reshape(slots, edge, edge),
        block_rows.reshape(1, slots),
        block_cols.reshape(1, slots),
        block_count.reshape(1),
        dangling.reshape(span // 128, 128),
        start_ranks.reshape(span // 128, 128),
    )
    ranks, resid = pl.pallas_call(
        finish,
        out_shape=(
            jax.ShapeDtypeStruct((span // 128, 128), f32),
            jax.ShapeDtypeStruct((1, ITERS), f32),
        ),
        in_specs=[vmem, vmem],
        out_specs=(vmem, vmem),
        compiler_params=pltpu.CompilerParams(vmem_limit_bytes=4 * 1024 * 1024),
    )(ranks, resid)
    return ranks.reshape(1, 1, 1, span), resid.T


def solution(mesh):
    placed = (
        P("layer", "row", "col", None, None, None),
        P("layer", "row", "col", None),
        P("layer", "row", "col", None),
        P("layer", "row", "col"),
        P("layer", "row", "col", None),
        P("layer", "row", "col", None),
    )
    return jax.shard_map(
        local,
        mesh=mesh,
        in_specs=placed,
        out_specs=(P("layer", "row", "col", None), P(None, "layer")),
        check_vma=False,
    )
```

```python
import functools

import jax
import jax.numpy as jnp
from jax import lax
from jax.experimental import pallas as pl
from jax.experimental.pallas import tpu as pltpu
from jax.sharding import PartitionSpec as P

ITERS = 3
CHUNK = 16

damping = 0.85
coupling = 0.3


def fold(v):
    rows, lanes = v.shape
    acc = v[:, 0:128]
    for h in range(1, lanes // 128):
        acc = acc + v[:, h * 128 : (h + 1) * 128]
    return jnp.sum(acc.reshape(rows // 8, 8, 128), axis=0)


def split(v):
    hi = v.astype(jnp.bfloat16)
    lo = (v - hi.astype(jnp.float32)).astype(jnp.bfloat16)
    return hi, lo


def dot(a, b):
    return jnp.dot(a, b, preferred_element_type=jnp.float32)


def kernel(
    nl, nr, nc, nodes,
    values_hbm, rows_ref, cols_ref, count_ref, dang_hbm, start_hbm,
    ranks_ref, resid_ref,
    values, dang_in, start_in, x_ref, inv_ref, kinv_ref,
    colsum, ohrow, ohcol, own_prod, chg,
    px_recv, pd_recv, col_send, col_recv, cs_recv, row_send, row_recv,
    sc_send, sc_recv, ma_send, ma_recv,
    pr_send, pr_recv, sp_send, sp_recv, rs_send, rs_recv,
    sem_in, sem_v,
    px_ss, px_rs, pd_ss, pd_rs, col_ss, col_rs, cs_ss, cs_rs, row_ss, row_rs, sc_ss, sc_rs, ma_ss, ma_rs,
    pr_ss, pr_rs, sp_ss, sp_rs, rs_ss, rs_rs,
):
    l, r, c = (lax.axis_index(a) for a in ("layer", "row", "col"))
    slots, edge, _ = values.shape
    blocks = x_ref.shape[0]
    halves = edge // 128
    nchunk = slots // CHUNK
    f32, bf16 = jnp.float32, jnp.bfloat16

    def remote(src, dst, ss, rs, ll, rr, cc):
        return pltpu.make_async_remote_copy(
            src_ref=src, dst_ref=dst, send_sem=ss, recv_sem=rs,
            device_id=(ll, rr, cc), device_id_type=pl.DeviceIdType.MESH,
        )

    in_d = pltpu.make_async_copy(dang_hbm, dang_in, sem_in.at[0])
    in_x = pltpu.make_async_copy(start_hbm, start_in, sem_in.at[1])
    vcopies = [
        pltpu.make_async_copy(
            values_hbm.at[pl.ds(k * CHUNK, CHUNK)], values.at[pl.ds(k * CHUNK, CHUNK)], sem_v.at[k]
        )
        for k in range(nchunk)
    ]
    in_x.start()
    in_d.start()
    for cp in vcopies:
        cp.start()

    peers = [(dr, dc) for dr in range(nr) for dc in range(nc) if (dr, dc) != (0, 0)]
    barrier = pltpu.get_barrier_semaphore()
    for dr, dc in peers:
        pl.semaphore_signal(
            barrier, inc=1,
            device_id=(l, lax.rem(r + dr, nr), lax.rem(c + dc, nc)),
            device_id_type=pl.DeviceIdType.MESH,
        )

    @pl.when(l > 0)
    def _():
        pl.semaphore_signal(
            barrier, inc=1, device_id=(l - 1, r, c), device_id_type=pl.DeviceIdType.MESH)

    @pl.when(l < nl - 1)
    def _():
        pl.semaphore_signal(
            barrier, inc=1, device_id=(l + 1, r, c), device_id_type=pl.DeviceIdType.MESH)

    live = lax.broadcasted_iota(jnp.int32, (1, slots), 1) < count_ref[...]
    rows = jnp.where(live, rows_ref[...], -1)
    cols = jnp.where(live, cols_ref[...], -1)
    row_send[...] = jnp.broadcast_to(
        jnp.concatenate([rows, jnp.full((1, 128 - slots), -1, jnp.int32)], axis=1), (8, 128)
    ).astype(f32)
    col_send[...] = jnp.broadcast_to(
        jnp.concatenate([cols, jnp.full((1, 128 - slots), -1, jnp.int32)], axis=1), (8, 128)
    ).astype(f32)

    eye = lax.broadcasted_iota(jnp.int32, (slots, slots), 0) == lax.broadcasted_iota(
        jnp.int32, (slots, slots), 1)
    colv = jnp.sum(
        jnp.where(eye, jnp.broadcast_to(cols_ref[...], (slots, slots)).astype(f32), 0.0),
        axis=1, keepdims=True,
    )
    for d in range(nr):
        base = lax.rem(r - d + nr, nr) * blocks
        at = (lax.broadcasted_iota(jnp.int32, (slots, blocks), 1) + base).astype(f32)
        ohcol[d] = jnp.where(colv == at, 1.0, 0.0).astype(bf16)

    ones = jnp.ones((CHUNK, edge), bf16)
    rid = lax.broadcasted_iota(jnp.int32, (CHUNK, edge), 0)

    def column_sum(k):
        vcopies[k].wait()
        acc = jnp.zeros((CHUNK, edge), f32)
        for s in range(CHUNK):
            acc = jnp.where(rid == s, dot(ones, values[k * CHUNK + s]), acc)
        colsum[k] = acc

    in_x.wait()
    in_d.wait()
    for h in range(halves):
        x_ref[:, h * 128 : (h + 1) * 128] = start_in[pl.ds(h, blocks, stride=halves), :]
    column_sum(0)

    order = []
    first, last = jnp.int32(0), jnp.int32(nc - 1)
    for _ in range(nc - 1):
        left = (c - first >= last - c).astype(jnp.int32)
        order.append(left * first + (1 - left) * last)
        first, last = first + left, last - (1 - left)
    far = [(cc, lax.rem(cc - c + nc, nc)) for cc in order]
    far_peers = [(dr, cc, d) for cc, d in far for dr in range(nr)]
    far_peers += [(dr, c, 0) for dr in range(1, nr)]
    sent = []

    pl.semaphore_wait(
        barrier, len(peers) + (l > 0).astype(jnp.int32) + (l < nl - 1).astype(jnp.int32))

    px, pd, pc, pcs, prow = [], [], [], [], []
    for d in range(1, nr):
        rr = lax.rem(r + d, nr)
        px.append(remote(start_in, px_recv.at[d], px_ss.at[d], px_rs.at[d], l, rr, c))
        pd.append(remote(dang_in, pd_recv.at[d], pd_ss.at[d], pd_rs.at[d], l, rr, c))
        pc.append(remote(col_send, col_recv.at[d], col_ss.at[d], col_rs.at[d], l, rr, c))
        pcs.append([
            remote(colsum.at[k], cs_recv.at[d, k], cs_ss.at[d, k], cs_rs.at[d, k], l, rr, c)
            for k in range(nchunk)
        ])
    for cc, d in far:
        prow.append(remote(row_send, row_recv.at[d], row_ss.at[d], row_rs.at[d], l, r, cc))
    for cp in px + pd + pc + prow + [q[0] for q in pcs]:
        cp.start()

    def spill_copies(t):
        return (
            remote(sp_send.at[t], sp_recv.at[t, 0], sp_ss.at[t, 0], sp_rs.at[t, 0], l + 1, r, c),
            remote(sp_send.at[t], sp_recv.at[t, 1], sp_ss.at[t, 1], sp_rs.at[t, 1], l - 1, r, c),
        )

    spread = jnp.where((l == 0) | (l == nl - 1), 1.0, 0.5).astype(f32) * coupling

    def send_spill(t, x):
        sp_send[t] = (x * spread).astype(sp_send.dtype)
        up, down = spill_copies(t)

        @pl.when(l < nl - 1)
        def _():
            up.start()

        @pl.when(l > 0)
        def _():
            down.start()

    @pl.when(l == 0)
    def _():
        for t in range(ITERS):
            sp_recv[t, 0] = jnp.zeros((blocks, edge), sp_recv.dtype)

    @pl.when(l == nl - 1)
    def _():
        for t in range(ITERS):
            sp_recv[t, 1] = jnp.zeros((blocks, edge), sp_recv.dtype)

    send_spill(0, x_ref[...])

    for k in range(1, nchunk):
        column_sum(k)
        for q in pcs:
            q[k].start()

    def spread_sums(tab, sums, rr):
        at = (lax.broadcasted_iota(jnp.int32, (blocks, slots), 0) + rr * blocks).astype(f32)
        oh = jnp.where(
            jnp.broadcast_to(tab[0:1, 0:slots], (blocks, slots)) == at, 1.0, 0.0).astype(bf16)
        hi, lo = split(sums.reshape(slots, edge))
        return dot(oh, hi) + dot(oh, lo)

    def piece(buf, h):
        return buf[pl.ds(h, blocks, stride=halves), :]

    near = [spread_sums(col_send, colsum[...], lax.rem(r - d + nr, nr)) for d in range(nr)]
    for cp in px + pd + pc:
        cp.wait_recv()
    peer_x = {d: jnp.concatenate([piece(px_recv.at[d], h) for h in range(halves)], axis=1)
              for d in range(1, nr)}
    keeps = {d: 1.0 - jnp.concatenate(
        [piece(pd_recv.at[d] if d else dang_in, h) for h in range(halves)], axis=1).astype(f32)
        for d in range(nr)}
    for q in pcs:
        for cp in q:
            cp.wait_recv()
    for d in range(nr):
        deg = near[d]
        for e in range(1, nr):
            deg = deg + spread_sums(col_recv[e], cs_recv[e], lax.rem(r - d + nr, nr))
        inv = 1.0 / (keeps[d] * deg + 1.0)
        kinv = keeps[d] * inv
        if d == 0:
            inv_ref[...] = inv
            kinv_ref[...] = kinv
        else:
            sc_recv[0, d] = (peer_x[d] * kinv).astype(bf16)

    def row_onehot(tab):
        at = (lax.broadcasted_iota(jnp.int32, (blocks, slots), 0) + c * blocks).astype(f32)
        return jnp.where(jnp.broadcast_to(tab[0:1, 0:slots], (blocks, slots)) == at,
                         1.0, 0.0).astype(bf16)

    def step(t):
        x = x_ref[...]
        scaled = (x * kinv_ref[...]).astype(bf16)
        if t > 0:
            sc_send[t] = scaled
        sc = [
            remote(sc_send.at[t], sc_recv.at[t, d], sc_ss.at[t, d], sc_rs.at[t, d],
                   l, lax.rem(r + d, nr), c)
            for d in range(1, nr)
            if t > 0
        ]
        for cp in sc:
            cp.start()
        mass_own = jnp.sum(fold(x * inv_ref[...]), axis=0, keepdims=True)
        ma_send[t] = mass_own
        ma = []
        for i, (dr, cc, dc) in enumerate(far_peers):
            slot = dr * nc + dc - 1
            ma.append(remote(ma_send.at[t], ma_recv.at[t, slot], ma_ss.at[t, slot],
                             ma_rs.at[t, slot], l, lax.rem(r + dr, nr), cc))
        for cp in ma:
            cp.start()

        if t > 0:
            send_spill(t, x)

        picked = dot(ohcol[0], scaled)
        for d in range(1, nr):
            if t > 0:
                sc[d - 1].wait_recv()
            picked = picked + dot(ohcol[d], sc_recv[t, d])
        picked = picked.astype(bf16)

        pr = []
        for k in range(nchunk):
            lhs = picked[k * CHUNK : (k + 1) * CHUNK]
            acc = jnp.zeros((CHUNK, edge), f32)
            for s in range(CHUNK):
                res = lax.dot_general(
                    lhs, values[k * CHUNK + s], (((1,), (1,)), ((), ())),
                    preferred_element_type=f32)
                acc = jnp.where(rid == s, res, acc)
            own_prod[k * CHUNK : (k + 1) * CHUNK] = acc
            pr_send[t, k] = acc.astype(pr_send.dtype)
            for cc, d in far:
                cp = remote(pr_send.at[t, k], pr_recv.at[t, d, k], pr_ss.at[t, d, k],
                            pr_rs.at[t, d, k], l, r, cc)
                cp.start()
                pr.append(cp)

        if t == 0:
            ohrow[0] = row_onehot(row_send)
            for cp in prow:
                cp.wait_recv()
            for d in range(1, nc):
                ohrow[d] = row_onehot(row_recv[d])

        phi, plo = split(own_prod[...])
        walk = dot(ohrow[0], phi) + dot(ohrow[0], plo)

        up, down = spill_copies(t)

        @pl.when(l > 0)
        def _():
            up.wait_recv()

        @pl.when(l < nl - 1)
        def _():
            down.wait_recv()

        arrive = sp_recv[t, 0].astype(f32) + sp_recv[t, 1].astype(f32)
        mass = mass_own
        for cp in ma:
            cp.wait_recv()
        for i in range(len(peers)):
            mass = mass + ma_recv[t, i]
        rest = damping * ((1.0 - coupling) * (jnp.sum(mass) / nodes) + arrive) + (1.0 - damping)

        for d in range(1, nc):
            for k in range(nchunk):
                remote(pr_send.at[t, k], pr_recv.at[t, d, k], pr_ss.at[t, d, k], pr_rs.at[t, d, k], l, r, lax.rem(c + d, nc)).wait_recv()
            got = pr_recv[t, d].reshape(slots, edge)
            if got.dtype == bf16:
                walk = walk + dot(ohrow[d], got)
            else:
                ghi, glo = split(got)
                walk = walk + dot(ohrow[d], ghi) + dot(ohrow[d], glo)
        updated = damping * (1.0 - coupling) * walk + rest
        x_ref[...] = updated
        chg[t] = fold(jnp.abs(updated - x))

        sent.extend(sc + ma + pr)

    for t in range(ITERS):
        step(t)

    lane = lax.broadcasted_iota(jnp.int32, (1, 128), 1)
    changes = jnp.zeros((1, 128), f32)
    for t in range(ITERS):
        changes = jnp.where(lane == t, jnp.sum(chg[t]), changes)
    rs_send[...] = changes
    rs = []
    for dr, cc, dc in far_peers:
        i = dr * nc + dc - 1
        cp = remote(rs_send, rs_recv.at[i], rs_ss.at[i], rs_rs.at[i],
                    l, lax.rem(r + dr, nr), cc)
        cp.start()
        rs.append(cp)
    for h in range(halves):
        ranks_ref[pl.ds(h, blocks, stride=halves), :] = x_ref[:, h * 128 : (h + 1) * 128]
    for cp in px + pd + pc + prow + [e for q in pcs for e in q] + sent:
        cp.wait_send()
    ups = [spill_copies(t) for t in range(ITERS)]

    @pl.when(l < nl - 1)
    def _():
        for up, _ in ups:
            up.wait_send()

    @pl.when(l > 0)
    def _():
        for _, down in ups:
            down.wait_send()

    total = rs_send[...]
    for cp in rs:
        cp.wait_recv()
    for i in range(len(peers)):
        total = total + rs_recv[i]
    resid_ref[...] = total
    for cp in rs:
        cp.wait_send()


def finish(ranks_in, resid_in, ranks_ref, resid_ref):
    ranks_ref[...] = ranks_in[...]
    resid_ref[...] = resid_in[:, 0:ITERS]


def local(block_values, block_rows, block_cols, block_count, dangling, start_ranks):
    span = start_ranks.shape[-1]
    nl, nr, nc = (lax.axis_size(a) for a in ("layer", "row", "col"))
    slots, edge = block_values.shape[3], block_values.shape[-1]
    blocks = span // edge
    nchunk = slots // CHUNK
    nodes = nr * nc * span
    npeer = nr * nc - 1
    f32, bf16 = jnp.float32, jnp.bfloat16
    vm, dma = pltpu.VMEM, pltpu.SemaphoreType.DMA
    big = (blocks, edge)
    PT, ST = bf16, f32
    scratch = [
        vm((slots, edge, edge), bf16), vm((span // 128, 128), jnp.int32), vm((span // 128, 128), f32),
        vm(big, f32), vm(big, f32), vm(big, f32),
        vm((nchunk, CHUNK, edge), f32), vm((nc, blocks, slots), bf16), vm((nr, slots, blocks), bf16),
        vm((slots, edge), f32), vm((ITERS, 8, 128), f32),
        vm((nr, span // 128, 128), f32), vm((nr, span // 128, 128), jnp.int32),
        vm((8, 128), f32), vm((nr, 8, 128), f32), vm((nr, nchunk, CHUNK, edge), f32),
        vm((8, 128), f32), vm((nc, 8, 128), f32),
        vm((ITERS,) + big, bf16), vm((ITERS, nr) + big, bf16),
        vm((ITERS, 1, 128), f32), vm((ITERS, npeer, 1, 128), f32),
        vm((ITERS, nchunk, CHUNK, edge), PT), vm((ITERS, nc, nchunk, CHUNK, edge), PT),
        vm((ITERS,) + big, ST), vm((ITERS, 2) + big, ST),
        vm((1, 128), f32), vm((npeer, 1, 128), f32),
        dma((2,)), dma((nchunk,)),
        dma((nr,)), dma((nr,)), dma((nr,)), dma((nr,)), dma((nr,)), dma((nr,)),
        dma((nr, nchunk)), dma((nr, nchunk)), dma((nc,)), dma((nc,)),
        dma((ITERS, nr)), dma((ITERS, nr)), dma((ITERS, npeer)), dma((ITERS, npeer)),
        dma((ITERS, nc, nchunk)), dma((ITERS, nc, nchunk)),
        dma((ITERS, 2)), dma((ITERS, 2)), dma((npeer,)), dma((npeer,)),
    ]
    hbm = pl.BlockSpec(memory_space=pltpu.HBM)
    vmem = pl.BlockSpec(memory_space=pltpu.VMEM)
    ranks, resid = pl.pallas_call(
        functools.partial(kernel, nl, nr, nc, nodes),
        out_shape=(
            pltpu.VMEM((span // 128, 128), f32),
            pltpu.VMEM((1, 128), f32),
        ),
        in_specs=[hbm, vmem, vmem, vmem, hbm, hbm],
        out_specs=(vmem, vmem),
        scratch_shapes=scratch,
        compiler_params=pltpu.CompilerParams(collective_id=0, has_side_effects=True),
    )(
        block_values.reshape(slots, edge, edge),
        block_rows.reshape(1, slots),
        block_cols.reshape(1, slots),
        block_count.reshape(1, 1),
        dangling.reshape(span // 128, 128),
        start_ranks.reshape(span // 128, 128),
    )
    ranks, resid = pl.pallas_call(
        finish,
        out_shape=(
            jax.ShapeDtypeStruct((span // 128, 128), f32),
            jax.ShapeDtypeStruct((1, ITERS), f32),
        ),
        in_specs=[vmem, vmem],
        out_specs=(vmem, vmem),
        compiler_params=pltpu.CompilerParams(vmem_limit_bytes=4 * 1024 * 1024),
    )(ranks, resid)
    return ranks.reshape(1, 1, 1, span), resid.T


def solution(mesh):
    placed = (
        P("layer", "row", "col", None, None, None),
        P("layer", "row", "col", None),
        P("layer", "row", "col", None),
        P("layer", "row", "col"),
        P("layer", "row", "col", None),
        P("layer", "row", "col", None),
    )
    return jax.shard_map(
        local,
        mesh=mesh,
        in_specs=placed,
        out_specs=(P("layer", "row", "col", None), P(None, "layer")),
        check_vma=False,
    )
```
